128 devices in a mesh: rep: 1, r: 4 (over x), s: 32 (over y, z, core).
Axes of the slice: x: 4, y: 4, z: 4, core: 2. Of those that a mesh axis runs over, the one named last changes fastest.
Arguments:
- x: bfloat16 [128, 2048, 1152], P(('rep', 'r', 's'))
- dy: bfloat16 [128, 2048, 1152], P(('rep', 'r', 's'))
- w_gate: bfloat16 [2, 1152, 4608], P(None, 's')
- w_up: bfloat16 [2, 1152, 4608], P(None, 's')
- w_down: bfloat16 [2, 4608, 1152], P(None, 's')
- m_w_gate: float32 [2, 1152, 4608], P(None, 's')
- m_w_up: float32 [2, 1152, 4608], P(None, 's')
- m_w_down: float32 [2, 4608, 1152], P(None, 's')
- v_w_gate: float32 [2, 1152, 4608], P(None, 's')
- v_w_up: float32 [2, 1152, 4608], P(None, 's')
- v_w_down: float32 [2, 4608, 1152], P(None, 's')
Outputs:
- output 1: bfloat16 [2, 1152, 4608], P('rep', 's')
- output 2: bfloat16 [2, 1152, 4608], P('rep', 's')
- output 3: bfloat16 [2, 4608, 1152], P('rep', 's')
- output 4: float32 [2, 1152, 4608], P('rep', 's')
- output 5: float32 [2, 1152, 4608], P('rep', 's')
- output 6: float32 [2, 4608, 1152], P('rep', 's')
- output 7: float32 [2, 1152, 4608], P('rep', 's')
- output 8: float32 [2, 1152, 4608], P('rep', 's')
- output 9: float32 [2, 4608, 1152], P('rep', 's')
All inputs are finite; a program needn't handle non-finite values.
Results may differ from the reference program's by a relative error of at most 0.022.
Values are sent between devices in bfloat16 or wider.
A program may use at most 1.5 GiB of HBM per device.

```python
import jax
import jax.numpy as jnp
from jax import lax

SEQUENCES = 128
TOKENS = 2048
D = 1152
FF = 4608
LAYERS = 2
NAMES = ("w_gate", "w_up", "w_down")
SHAPES = {"w_gate": (LAYERS, D, FF), "w_up": (LAYERS, D, FF), "w_down": (LAYERS, FF, D)}


def bump(key, n, height):
    away = (jnp.arange(n, dtype=jnp.int32) - jax.random.randint(key, (), 0, n, jnp.int32)) % n
    return jnp.where(away < n // 8, height, 1.0)


def together(key, own, strength):
    shared = jax.random.normal(key, own.shape[1:], jnp.float32)
    return (own + strength * shared) * lax.rsqrt(1 + strength * strength)


def setup_inputs(seed: int = 0, part: int = 0) -> dict:
    kx, kdy, ka, kb, kz, kf, kh, kl, *keys = jax.random.split(jax.random.key(seed), 8 + 3 * len(NAMES))
    kx, kdy, ka, kb = (jax.random.fold_in(k, part) for k in (kx, kdy, ka, kb))
    kw, km, kv = (keys[i::3] for i in range(3))
    shape = (SEQUENCES, TOKENS, D)
    much_x, much_dy = jax.random.uniform(kz, (2,), jnp.float32, 0.0, 1.0)
    loud = 2.0 ** jax.random.uniform(jax.random.fold_in(kz, 1), (), jnp.float32, -1.0, 2.0)
    layers = 2.0 ** jax.random.uniform(kl, (LAYERS, 1, 1), jnp.float32, -1.0, 1.0)
    x = together(ka, jax.random.normal(kx, shape, jnp.float32), much_x) * bump(kf, D, 4.0)
    dy = together(kb, jax.random.normal(kdy, shape, jnp.float32), much_dy)
    drawn = {"x": x.astype(jnp.bfloat16), "dy": (loud * dy * (SEQUENCES * TOKENS) ** -0.5).astype(jnp.bfloat16)}
    for key, name in zip(kw, NAMES, strict=True):
        w = jax.random.normal(key, SHAPES[name], jnp.float32) * SHAPES[name][1] ** -0.5
        drawn[name] = (w * {"w_gate": 1.0, "w_up": bump(kh, FF, 4.0), "w_down": layers}[name]).astype(jnp.bfloat16)
    for key, name in zip(km, NAMES, strict=True):
        drawn[f"m_{name}"] = 0.1 * jax.random.normal(key, SHAPES[name], jnp.float32)
    for key, name in zip(kv, NAMES, strict=True):
        drawn[f"v_{name}"] = jax.random.uniform(key, SHAPES[name], jnp.float32, 0.005, 0.015)
    return drawn


def matmul(a, w):
    return jnp.dot(a, w, preferred_element_type=jnp.float32).astype(jnp.bfloat16)


def normed(h):
    wide = h.astype(jnp.float32)
    scale = lax.rsqrt(jnp.mean(wide**2, -1, keepdims=True) + 1e-6)
    return (wide * scale).astype(jnp.bfloat16)


def layer(h, w):
    a = normed(h)
    gate = jnp.dot(a, w["w_gate"], preferred_element_type=jnp.float32)
    up = jnp.dot(a, w["w_up"], preferred_element_type=jnp.float32)
    return h + matmul((jax.nn.silu(gate) * up).astype(jnp.bfloat16), w["w_down"])


def adamw(w, m, v, g):
    m = 0.9 * m + 0.1 * g
    v = 0.95 * v + 0.05 * g * g
    step = m * lax.rsqrt(v + 1e-8) + 0.1 * w
    return (w - 0.02 * step).astype(jnp.bfloat16), m, v


def clipped(gradients, sum_of_squares, count):
    factor = jnp.minimum(1.0, 0.5 * lax.rsqrt(sum_of_squares / count + 1e-30))
    return [g * factor for g in gradients]


def stack(weights, h):
    return lax.scan(lambda h, w: (layer(h, w), None), h, weights)[0]


def reference(x, dy, w_gate, w_up, w_down, m_w_gate, m_w_up, m_w_down, v_w_gate, v_w_up, v_w_down):
    weights = dict(zip(NAMES, (w_gate, w_up, w_down), strict=True))

    def take(so_far, sequence):
        h, by_y = sequence
        _, back = jax.vjp(lambda w: stack(w, h), weights)
        return jax.tree.map(lambda total, term: total + term.astype(jnp.float32), so_far, back(by_y)[0]), None

    none_yet = {name: jnp.zeros(w.shape, jnp.float32) for name, w in weights.items()}
    by_weights, _ = lax.scan(take, none_yet, (x, dy))
    gradients = [by_weights[name].astype(jnp.bfloat16).astype(jnp.float32) for name in NAMES]
    gradients = clipped(gradients, sum(jnp.sum(g * g) for g in gradients), sum(g.size for g in gradients))
    new = [
        adamw(w.astype(jnp.float32), m, v, g)
        for w, m, v, g in zip((w_gate, w_up, w_down), (m_w_gate, m_w_up, m_w_down), (v_w_gate, v_w_up, v_w_down), gradients, strict=True)
    ]
    return tuple(one[which] for which in range(3) for one in new)
```

```python
import functools

import jax
import jax.numpy as jnp
from jax import lax
from jax.experimental import pallas as pl
from jax.experimental.pallas import tpu as pltpu
from jax.sharding import PartitionSpec as P

BF, F32 = jnp.bfloat16, jnp.float32
S = 32
D, FF, T = 1152, 4608, 2048
C = 1152
Q = FF // C
ROWS = 432
LIMIT = 62 * 1024 * 1024
LAST, FIRST = ((1,), (1,)), ((0,), (0,))


def params(dims):
    return pltpu.CompilerParams(dimension_semantics=("arbitrary",) * dims, vmem_limit_bytes=LIMIT)


def cost(flops, moved):
    return pl.CostEstimate(flops=int(flops), bytes_accessed=int(moved), transcendentals=0)


def dot(a, b):
    return jnp.dot(a, b, preferred_element_type=F32)


def dot_general(a, b, dims):
    return lax.dot_general(a, b, (dims, ((), ())), preferred_element_type=F32)


def assemble(to, main, rest):
    to[0:1024, :] = main[...].reshape(1024, C)
    to[1024:1152, :] = rest[...]


def normed_wide(wide):
    return wide * lax.rsqrt(jnp.mean(wide * wide, -1, keepdims=True) + 1e-6)


def gate_up_kernel(a_ref, g_ref, u_ref, gr_ref, ur_ref, act_ref, wg, wu):
    @pl.when(pl.program_id(1) == 0)
    def _():
        assemble(wg, g_ref, gr_ref)
        assemble(wu, u_ref, ur_ref)

    a = a_ref[...]
    gate, up = dot(a, wg[...]), dot(a, wu[...])
    act_ref[...] = (gate * jax.nn.sigmoid(gate) * up).astype(BF)


def weight_specs():
    return [
        pl.BlockSpec((S, 32, C), lambda q, i: (0, q, 0)),
        pl.BlockSpec((S, 32, C), lambda q, i: (0, Q + q, 0)),
        pl.BlockSpec((128, C), lambda q, i: (q, 0)),
        pl.BlockSpec((128, C), lambda q, i: (Q + q, 0)),
    ]


def gate_up(a, packed, rest, tm=512):
    return pl.pallas_call(
        gate_up_kernel,
        out_shape=jax.ShapeDtypeStruct((T, FF), BF),
        grid=(Q, T // tm),
        in_specs=[pl.BlockSpec((tm, D), lambda q, i: (i, 0))] + weight_specs(),
        out_specs=pl.BlockSpec((tm, C), lambda q, i: (i, q)),
        scratch_shapes=[pltpu.VMEM((D, C), BF)] * 2,
        compiler_params=params(2),
        cost_estimate=cost(4 * T * D * FF, 60e6),
        name="gate_up",
    )(a, packed, packed, rest, rest)


def down_kernel(act_ref, w_ref, x_ref, h_ref, a_ref):
    out = dot(act_ref[...], w_ref[...].reshape(FF, D)).astype(BF)
    h = x_ref[...] + out
    h_ref[...] = h
    a_ref[...] = normed_wide(h.astype(F32)).astype(BF)


def down(act, packed, x, tm=256):
    row = pl.BlockSpec((tm, D), lambda i: (i, 0))
    return pl.pallas_call(
        down_kernel,
        out_shape=(jax.ShapeDtypeStruct((T, D), BF),) * 2,
        grid=(T // tm,),
        in_specs=[pl.BlockSpec((tm, FF), lambda i: (i, 0)), pl.BlockSpec((S, 144, D), lambda i: (0, 2, 0)), row],
        out_specs=(row, row),
        compiler_params=params(1),
        cost_estimate=cost(2 * T * D * FF, 45e6),
        name="down",
    )(act, packed, x)


def back_kernel(with_act, a_ref, dy_ref, g_ref, u_ref, gr_ref, ur_ref, d_ref, *refs):
    if with_act:
        act_ref, dgu_ref, wg, wu = refs
    else:
        dgu_ref, wg, wu = refs

    @pl.when(pl.program_id(1) == 0)
    def _():
        assemble(wg, g_ref, gr_ref)
        assemble(wu, u_ref, ur_ref)

    a = a_ref[...]
    gate, up = dot(a, wg[...]), dot(a, wu[...])
    dact = dot_general(dy_ref[...], d_ref[...].reshape(C, D), LAST).astype(BF).astype(F32)
    sig = jax.nn.sigmoid(gate)
    silu = gate * sig
    if with_act:
        act_ref[...] = (silu * up).astype(BF)
    dgu_ref[0, :, :] = (dact * up * (sig + silu * (1.0 - sig))).astype(BF)
    dgu_ref[1, :, :] = (dact * silu).astype(BF)


def back(a, dy, packed, rest, with_act, tm=512):
    row = pl.BlockSpec((tm, D), lambda q, i: (i, 0))
    shapes = [jax.ShapeDtypeStruct((2, T, FF), BF)]
    specs = [pl.BlockSpec((2, tm, C), lambda q, i: (0, i, q))]
    if with_act:
        shapes.insert(0, jax.ShapeDtypeStruct((T, FF), BF))
        specs.insert(0, pl.BlockSpec((tm, C), lambda q, i: (i, q)))
    out = pl.pallas_call(
        functools.partial(back_kernel, with_act),
        out_shape=tuple(shapes),
        grid=(Q, T // tm),
        in_specs=[row, row] + weight_specs() + [pl.BlockSpec((8, 144, D), lambda q, i: (q, 2, 0))],
        out_specs=tuple(specs),
        scratch_shapes=[pltpu.VMEM((D, C), BF)] * 2,
        compiler_params=params(2),
        cost_estimate=cost(6 * T * D * FF, 130e6),
        name="back",
    )(a, dy, packed, packed, rest, rest, packed)
    return out if with_act else (None, out[0])


def dstate_kernel(dg_ref, du_ref, g_ref, u_ref, gr_ref, ur_ref, h_ref, dy_ref, dh_ref, wg, wu, sg, su, *, tm):
    q, i = pl.program_id(0), pl.program_id(1)

    @pl.when(i == 0)
    def _():
        assemble(wg, g_ref, gr_ref)
        assemble(wu, u_ref, ur_ref)

    rows = pl.ds(pl.multiple_of(i * tm, tm), tm)
    pg, pu = dot_general(dg_ref[0], wg[...], LAST), dot_general(du_ref[0], wu[...], LAST)

    @pl.when(q == 0)
    def _():
        sg[rows, :] = pg
        su[rows, :] = pu

    @pl.when(q > 0)
    def _():
        sg[rows, :] = sg[rows, :] + pg
        su[rows, :] = su[rows, :] + pu

    @pl.when(q == Q - 1)
    def _():
        da = (sg[rows, :].astype(BF) + su[rows, :].astype(BF)).astype(F32)
        wide = h_ref[...].astype(F32)
        scale = lax.rsqrt(jnp.mean(wide * wide, -1, keepdims=True) + 1e-6)
        along = jnp.sum(da * wide, -1, keepdims=True) * (scale * scale * scale) * (1.0 / D)
        dh_ref[...] = dy_ref[...] + (da * scale - wide * along).astype(BF)


def dstate(dgu, packed, rest, h, dy, tm=512):
    last = pl.BlockSpec((tm, D), lambda q, i: (jnp.where(q == Q - 1, i, 0), 0))
    return pl.pallas_call(
        functools.partial(dstate_kernel, tm=tm),
        out_shape=jax.ShapeDtypeStruct((T, D), BF),
        grid=(Q, T // tm),
        in_specs=[pl.BlockSpec((1, tm, C), lambda q, i: (0, i, q)), pl.BlockSpec((1, tm, C), lambda q, i: (1, i, q))]
        + weight_specs()
        + [last, last],
        out_specs=last,
        scratch_shapes=[pltpu.VMEM((D, C), BF)] * 2 + [pltpu.VMEM((T, D), F32)] * 2,
        compiler_params=params(2),
        cost_estimate=cost(4 * T * D * FF, 75e6),
        name="dstate",
    )(dgu, dgu, packed, packed, rest, rest, h, dy)


def d_down_kernel(act_ref, dy_ref, out_ref):
    out_ref[...] = dot_general(act_ref[...], dy_ref[...], FIRST).astype(BF).reshape(8, 144, D)


def d_down(act, dy, alone):
    return pl.pallas_call(
        d_down_kernel,
        out_shape=jax.ShapeDtypeStruct((S, 144 if alone else ROWS, D), BF),
        grid=(Q,),
        in_specs=[pl.BlockSpec((T, C), lambda q: (0, q)), pl.BlockSpec((T, D), lambda q: (0, 0))],
        out_specs=pl.BlockSpec((8, 144, D), lambda q: (q, 0 if alone else 2, 0)),
        compiler_params=params(1),
        cost_estimate=cost(2 * T * D * FF, 35e6),
        name="d_down",
    )(act, dy)


def d_gate_up_kernel(at_ref, dgu_ref, order_ref, *refs):
    out_ref, rest = refs[-2:]
    g = pl.program_id(0)

    @pl.when(g < 2 * Q)
    def _():
        term = dot(at_ref[...], dgu_ref[0]).astype(BF)
        out_ref[...] = term[0:1024, :].reshape(S, 32, C)
        rest[pl.ds(pl.multiple_of(g * 128, 128), 128), :] = term[1024:1152, :]

    @pl.when(g == 2 * Q)
    def _():
        out_ref[...] = dot(order_ref[...], rest[...]).astype(BF).reshape(S, 32, C)


def d_gate_up(at, dgu, order, packed=None):
    def block(g):
        g = jnp.minimum(g, 2 * Q - 1)
        return (g // Q, 0, g % Q)

    return pl.pallas_call(
        d_gate_up_kernel,
        out_shape=jax.ShapeDtypeStruct((S, 288 if packed is None else ROWS, D), BF),
        grid=(2 * Q + 1,),
        in_specs=[
            pl.BlockSpec((D, T), lambda g: (0, 0)),
            pl.BlockSpec((1, T, C), block),
            pl.BlockSpec((1024, 1024), lambda g: (0, 0)),
        ]
        + [pl.BlockSpec(memory_space=pl.ANY)] * (packed is not None),
        out_specs=pl.BlockSpec((S, 32, C), lambda g: (0, g, 0)),
        scratch_shapes=[pltpu.VMEM((1024, C), BF)],
        input_output_aliases={} if packed is None else {3: 0},
        compiler_params=params(1),
        cost_estimate=cost(4 * T * D * FF, 65e6),
        name="d_gate_up",
    )(at, dgu, order, *([] if packed is None else [packed]))


def total_kernel(part_ref, out_ref, mine, slots, send, recv):
    me = lax.axis_index("s")
    y, z, core = me // 8, (me // 2) % 4, me % 2
    stages = [
        [y * 8 + z * 2 + (1 - core)],
        [y * 8 + ((z + k) % 4) * 2 + core for k in (1, 2, 3)],
        [((y + k) % 4) * 8 + z * 2 + core for k in (1, 2, 3)],
    ]
    barrier = pltpu.get_barrier_semaphore()
    for peers in stages:
        for peer in peers:
            pl.semaphore_signal(barrier, inc=1, device_id={"s": peer}, device_id_type=pl.DeviceIdType.MESH)
    pl.semaphore_wait(barrier, 7)
    total, slot = part_ref[...], 0
    for number, peers in enumerate(stages):
        mine[number] = total
        copies = []
        for peer in peers:
            copy = pltpu.make_async_remote_copy(
                src_ref=mine.at[number],
                dst_ref=slots.at[slot],
                send_sem=send.at[slot],
                recv_sem=recv.at[slot],
                device_id={"s": peer},
                device_id_type=pl.DeviceIdType.MESH,
            )
            copy.start()
            copies.append((copy, slot))
            slot += 1
        for copy, at in copies:
            copy.wait()
            total = total + slots[at]
    out_ref[...] = total


def summed_over_group(part):
    block = jnp.where(lax.broadcasted_iota(jnp.int32, (8, 128), 0) + lax.broadcasted_iota(jnp.int32, (8, 128), 1) == 0, part, 0.0)
    return pl.pallas_call(
        total_kernel,
        out_shape=jax.ShapeDtypeStruct((8, 128), F32),
        in_specs=[pl.BlockSpec(memory_space=pltpu.VMEM)],
        out_specs=pl.BlockSpec(memory_space=pltpu.VMEM),
        scratch_shapes=[
            pltpu.VMEM((3, 8, 128), F32),
            pltpu.VMEM((7, 8, 128), F32),
            pltpu.SemaphoreType.DMA((7,)),
            pltpu.SemaphoreType.DMA((7,)),
        ],
        compiler_params=pltpu.CompilerParams(collective_id=0, has_side_effects=True),
        name="total",
    )(block)[0, 0]


def one_hot(rows, columns):
    return (rows[:, None] == columns[None, :]).astype(BF)


def feature_order():
    j = jnp.arange(D, dtype=jnp.int32)
    k = j - 1024
    return one_hot(j, jnp.where(j < 1024, (j // 32) * 36 + j % 32, (k // 4) * 36 + 32 + k % 4))


def rest_order():
    p, t = (jnp.arange(1024, dtype=jnp.int32) for _ in range(2))
    return one_hot((p % 32 // 4) * 128 + (p // 32) * 4 + p % 4, t)


def moved(a, order):
    return jnp.dot(a, order, preferred_element_type=F32).astype(BF)


def pack(gate, up, dn, order):
    main = [w[:32].reshape(32, Q, C).transpose(1, 0, 2).reshape(128, C) for w in (gate, up)]
    rest = [w[32:].reshape(4, Q, C).transpose(1, 0, 2).reshape(16, C) for w in (gate, up)]
    return jnp.concatenate(main + rest + [moved(dn, order)])


def unpack(g, order):
    out = []
    for i in range(2):
        main = g[128 * i : 128 * i + 128].reshape(Q, 32, C).transpose(1, 0, 2).reshape(32, FF)
        rest = g[256 + 16 * i : 272 + 16 * i].reshape(Q, 4, C).transpose(1, 0, 2).reshape(4, FF)
        out.append(jnp.concatenate([main, rest]))
    return out + [moved(g[288:], order.T)]


def adamw(w, m, v, g):
    m = 0.9 * m + 0.1 * g
    v = 0.95 * v + 0.05 * g * g
    step = m * lax.rsqrt(v + 1e-8) + 0.1 * w
    return (w - 0.02 * step).astype(BF), m, v


def across(block, n=4):
    total = block.astype(F32)
    for shift in range(1, n):
        total = total + lax.ppermute(block, "r", [(i, (i + shift) % n) for i in range(n)]).astype(F32)
    return total.astype(BF)


def scattered(term):
    return lax.psum_scatter(term.reshape(-1, C), "s", scatter_dimension=0, tiled=True)


def rest_of(packed, rests):
    return moved(rests.T, packed[:, 256:288, :].reshape(1024, C))


def solution(mesh):
    def step(x, dy, *arrays):
        weights, m, v = (arrays[i : i + 3] for i in (0, 3, 6))
        order, rests = feature_order(), rest_order()

        packed = [
            lax.all_gather(pack(*(w[n] for w in weights), order), "s", axis=0, tiled=True).reshape(S, ROWS, C)
            for n in range(2)
        ]

        x, dy = moved(x[0], order), moved(dy[0], order)
        a0 = normed_wide(x.astype(F32)).astype(BF)
        at0 = a0.T
        rest = [rest_of(packed[0], rests)]
        act0 = gate_up(a0, packed[0], rest[0])
        h1, a1 = down(act0, packed[0], x)
        a1, packed[1] = lax.optimization_barrier((a1, packed[1]))
        rest.append(rest_of(packed[1], rests))
        at1 = a1.T
        act1, dgu1 = back(a1, dy, packed[1], rest[1], True)
        term1 = d_gate_up(at1, dgu1, rests, d_down(act1, dy, False))
        term1, dgu1 = lax.optimization_barrier((term1, dgu1))
        sum1 = scattered(term1)
        dh1 = dstate(dgu1, packed[1], rest[1], h1, dy)
        down0, dh1 = lax.optimization_barrier((d_down(act0, dh1, True), dh1))
        sum_down0 = scattered(down0)
        _, dgu0 = back(a0, dh1, packed[0], rest[0], False)
        sum0 = scattered(d_gate_up(at0, dgu0, rests))

        blocks = [across(b) for b in (sum0, sum_down0, sum1)]
        squares = summed_over_group(sum(jnp.sum(jnp.square(b.astype(F32))) for b in blocks))
        blocks = [jnp.concatenate(blocks[:2]), blocks[2]]
        factor = jnp.minimum(1.0, 0.5 * lax.rsqrt(squares / (2 * 3 * D * FF) + 1e-30))
        pieces = [unpack(b, order) for b in blocks]
        new = [
            adamw(weights[i].astype(F32), m[i], v[i], jnp.stack([pieces[n][i] for n in range(2)]).astype(F32) * factor)
            for i in range(3)
        ]
        return tuple(one[which] for which in range(3) for one in new)

    states, cut = P(("rep", "r", "s"), None, None), P(None, "s", None)
    return jax.shard_map(
        step,
        mesh=mesh,
        in_specs=(states, states) + (cut,) * 9,
        out_specs=(P("rep", "s", None),) * 9,
        check_vma=False,
    )
```

```python
import functools

import jax
import jax.numpy as jnp
from jax import lax
from jax.experimental import pallas as pl
from jax.experimental.pallas import tpu as pltpu
from jax.sharding import PartitionSpec as P


BF, F32 = jnp.bfloat16, jnp.float32
S = 32
D, FF, T = 1152, 4608, 2048
C = 1152
Q = FF // C
ROWS = 432
LIMIT = 62 * 1024 * 1024
CUTS = ((0, 512), (512, 1152))
LAST, FIRST = ((1,), (1,)), ((0,), (0,))


def params(dims):
    return pltpu.CompilerParams(dimension_semantics=("arbitrary",) * dims, vmem_limit_bytes=LIMIT)


def cost(flops, moved):
    return pl.CostEstimate(flops=int(flops), bytes_accessed=int(moved), transcendentals=0)


def dot(a, b):
    return jnp.dot(a, b, preferred_element_type=F32)


def dot_general(a, b, dims):
    return lax.dot_general(a, b, (dims, ((), ())), preferred_element_type=F32)


def assemble(to, main, rest):
    to[0:1024, :] = main[...].reshape(1024, C)
    to[1024:1152, :] = rest[...]


def normed_wide(wide):
    return wide * lax.rsqrt(jnp.mean(wide * wide, -1, keepdims=True) + 1e-6)


def gate_up_kernel(a_ref, g_ref, u_ref, gr_ref, ur_ref, act_ref, wg, wu):
    @pl.when(pl.program_id(1) == 0)
    def _():
        assemble(wg, g_ref, gr_ref)
        assemble(wu, u_ref, ur_ref)

    a = a_ref[...]
    for at, to in CUTS:
        gate, up = dot(a, wg[:, at:to]), dot(a, wu[:, at:to])
        act_ref[:, at:to] = (gate * jax.nn.sigmoid(gate) * up).astype(BF)


def weight_specs():
    return [
        pl.BlockSpec((S, 32, C), lambda q, i: (0, q, 0)),
        pl.BlockSpec((S, 32, C), lambda q, i: (0, Q + q, 0)),
        pl.BlockSpec((128, C), lambda q, i: (q, 0)),
        pl.BlockSpec((128, C), lambda q, i: (Q + q, 0)),
    ]


def gate_up(a, packed, rest, tm=512):
    return pl.pallas_call(
        gate_up_kernel,
        out_shape=jax.ShapeDtypeStruct((T, FF), BF),
        grid=(Q, T // tm),
        in_specs=[pl.BlockSpec((tm, D), lambda q, i: (i, 0))] + weight_specs(),
        out_specs=pl.BlockSpec((tm, C), lambda q, i: (i, q)),
        scratch_shapes=[pltpu.VMEM((D, C), BF)] * 2,
        compiler_params=params(2),
        cost_estimate=cost(4 * T * D * FF, 60e6),
        name="gate_up",
    )(a, packed, packed, rest, rest)


def down_kernel(act_ref, w_ref, x_ref, h_ref, a_ref):
    out = dot(act_ref[...], w_ref[...].reshape(FF, D)).astype(BF)
    h = x_ref[...] + out
    h_ref[...] = h
    a_ref[...] = normed_wide(h.astype(F32)).astype(BF)


def down(act, packed, x, tm=256):
    row = pl.BlockSpec((tm, D), lambda i: (i, 0))
    return pl.pallas_call(
        down_kernel,
        out_shape=(jax.ShapeDtypeStruct((T, D), BF),) * 2,
        grid=(T // tm,),
        in_specs=[pl.BlockSpec((tm, FF), lambda i: (i, 0)), pl.BlockSpec((S, 144, D), lambda i: (0, 2, 0)), row],
        out_specs=(row, row),
        compiler_params=params(1),
        cost_estimate=cost(2 * T * D * FF, 45e6),
        name="down",
    )(act, packed, x)


def back_kernel(with_act, a_ref, dy_ref, g_ref, u_ref, gr_ref, ur_ref, d_ref, *refs):
    if with_act:
        act_ref, dgu_ref, wg, wu, wd = refs
    else:
        dgu_ref, wg, wu, wd = refs

    @pl.when(pl.program_id(1) == 0)
    def _():
        assemble(wg, g_ref, gr_ref)
        assemble(wu, u_ref, ur_ref)
        wd[...] = d_ref[...].reshape(C, D)

    a, dy = a_ref[...], dy_ref[...]
    for at, to in CUTS:
        gate, up = dot(a, wg[:, at:to]), dot(a, wu[:, at:to])
        dact = dot_general(dy, wd[at:to, :], LAST).astype(BF).astype(F32)
        sig = jax.nn.sigmoid(gate)
        silu = gate * sig
        if with_act:
            act_ref[:, at:to] = (silu * up).astype(BF)
        dgu_ref[0, :, at:to] = (dact * up * (sig + silu * (1.0 - sig))).astype(BF)
        dgu_ref[1, :, at:to] = (dact * silu).astype(BF)


def back(a, dy, packed, rest, with_act, tm=512):
    row = pl.BlockSpec((tm, D), lambda q, i: (i, 0))
    shapes = [jax.ShapeDtypeStruct((2, T, FF), BF)]
    specs = [pl.BlockSpec((2, tm, C), lambda q, i: (0, i, q))]
    if with_act:
        shapes.insert(0, jax.ShapeDtypeStruct((T, FF), BF))
        specs.insert(0, pl.BlockSpec((tm, C), lambda q, i: (i, q)))
    out = pl.pallas_call(
        functools.partial(back_kernel, with_act),
        out_shape=tuple(shapes),
        grid=(Q, T // tm),
        in_specs=[row, row] + weight_specs() + [pl.BlockSpec((8, 144, D), lambda q, i: (q, 2, 0))],
        out_specs=tuple(specs),
        scratch_shapes=[pltpu.VMEM((D, C), BF)] * 3,
        compiler_params=params(2),
        cost_estimate=cost(6 * T * D * FF, 130e6),
        name="back",
    )(a, dy, packed, packed, rest, rest, packed)
    return out if with_act else (None, out[0])


def dstate_kernel(dg_ref, du_ref, g_ref, r_ref, h_ref, dy_ref, dh_ref, wg, wu):
    @pl.when(pl.program_id(0) == 0)
    def _():
        for q in range(Q):
            cols = slice(q * C, (q + 1) * C)
            wg[0:1024, cols] = g_ref[:, 32 * q : 32 * q + 32, :].reshape(1024, C)
            wu[0:1024, cols] = g_ref[:, 128 + 32 * q : 160 + 32 * q, :].reshape(1024, C)
            wg[1024:1152, cols] = r_ref[128 * q : 128 * q + 128, :]
            wu[1024:1152, cols] = r_ref[512 + 128 * q : 640 + 128 * q, :]

    pg, pu = dot_general(dg_ref[0], wg[...], LAST), dot_general(du_ref[0], wu[...], LAST)
    da = (pg.astype(BF) + pu.astype(BF)).astype(F32)
    wide = h_ref[...].astype(F32)
    scale = lax.rsqrt(jnp.mean(wide * wide, -1, keepdims=True) + 1e-6)
    along = jnp.sum(da * wide, -1, keepdims=True) * (scale * scale * scale) * (1.0 / D)
    dh_ref[...] = dy_ref[...] + (da * scale - wide * along).astype(BF)


def dstate(dgu, packed, rest, h, dy, tm=256):
    row = pl.BlockSpec((tm, D), lambda i: (i, 0))
    return pl.pallas_call(
        dstate_kernel,
        out_shape=jax.ShapeDtypeStruct((T, D), BF),
        grid=(T // tm,),
        in_specs=[
            pl.BlockSpec((1, tm, FF), lambda i: (0, i, 0)),
            pl.BlockSpec((1, tm, FF), lambda i: (1, i, 0)),
            pl.BlockSpec((S, 256, C), lambda i: (0, 0, 0), pipeline_mode=pl.Buffered(1)),
            pl.BlockSpec((1024, C), lambda i: (0, 0), pipeline_mode=pl.Buffered(1)),
            row,
            row,
        ],
        out_specs=row,
        scratch_shapes=[pltpu.VMEM((D, FF), BF)] * 2,
        compiler_params=params(1),
        cost_estimate=cost(4 * T * D * FF, 75e6),
        name="dstate",
    )(dgu, dgu, packed, rest, h, dy)


def d_down_kernel(act_ref, dy_ref, out_ref):
    out_ref[...] = dot_general(act_ref[...], dy_ref[...], FIRST).astype(BF).reshape(8, 144, D)


def d_down(act, dy):
    return pl.pallas_call(
        d_down_kernel,
        out_shape=jax.ShapeDtypeStruct((S, 144, D), BF),
        grid=(Q,),
        in_specs=[pl.BlockSpec((T, C), lambda q: (0, q)), pl.BlockSpec((T, D), lambda q: (0, 0))],
        out_specs=pl.BlockSpec((8, 144, D), lambda q: (q, 0, 0)),
        compiler_params=params(1),
        cost_estimate=cost(2 * T * D * FF, 35e6),
        name="d_down",
    )(act, dy)


def d_gate_up_kernel(at_ref, dgu_ref, order_ref, out_ref, rest):
    g = pl.program_id(0)

    @pl.when(g < 2 * Q)
    def _():
        term = dot(at_ref[...], dgu_ref[0]).astype(BF)
        out_ref[...] = term[0:1024, :].reshape(S, 32, C)
        rest[pl.ds(pl.multiple_of(g * 128, 128), 128), :] = term[1024:1152, :]

    @pl.when(g == 2 * Q)
    def _():
        out_ref[...] = dot(order_ref[...], rest[...]).astype(BF).reshape(S, 32, C)


def d_gate_up(at, dgu, order):
    def block(g):
        g = jnp.minimum(g, 2 * Q - 1)
        return (g // Q, 0, g % Q)

    return pl.pallas_call(
        d_gate_up_kernel,
        out_shape=jax.ShapeDtypeStruct((S, 288, D), BF),
        grid=(2 * Q + 1,),
        in_specs=[
            pl.BlockSpec((D, T), lambda g: (0, 0)),
            pl.BlockSpec((1, T, C), block),
            pl.BlockSpec((1024, 1024), lambda g: (0, 0)),
        ],
        out_specs=pl.BlockSpec((S, 32, C), lambda g: (0, g, 0)),
        scratch_shapes=[pltpu.VMEM((1024, C), BF)],
        compiler_params=params(1),
        cost_estimate=cost(4 * T * D * FF, 65e6),
        name="d_gate_up",
    )(at, dgu, order)


def total_kernel(part_ref, out_ref, mine, slots, send, recv):
    me = lax.axis_index("s")
    y, z, core = me // 8, (me // 2) % 4, me % 2
    stages = [
        [y * 8 + z * 2 + (1 - core)],
        [y * 8 + ((z + k) % 4) * 2 + core for k in (1, 2, 3)],
        [((y + k) % 4) * 8 + z * 2 + core for k in (1, 2, 3)],
    ]
    barrier = pltpu.get_barrier_semaphore()
    for peers in stages:
        for peer in peers:
            pl.semaphore_signal(barrier, inc=1, device_id={"s": peer}, device_id_type=pl.DeviceIdType.MESH)
    pl.semaphore_wait(barrier, 7)
    total, slot = part_ref[...], 0
    for number, peers in enumerate(stages):
        mine[number] = total
        copies = []
        for peer in peers:
            copy = pltpu.make_async_remote_copy(
                src_ref=mine.at[number],
                dst_ref=slots.at[slot],
                send_sem=send.at[slot],
                recv_sem=recv.at[slot],
                device_id={"s": peer},
                device_id_type=pl.DeviceIdType.MESH,
            )
            copy.start()
            copies.append((copy, slot))
            slot += 1
        for copy, at in copies:
            copy.wait()
            total = total + slots[at]
    out_ref[...] = total


def summed_over_group(part):
    block = jnp.where(lax.broadcasted_iota(jnp.int32, (8, 128), 0) + lax.broadcasted_iota(jnp.int32, (8, 128), 1) == 0, part, 0.0)
    return pl.pallas_call(
        total_kernel,
        out_shape=jax.ShapeDtypeStruct((8, 128), F32),
        in_specs=[pl.BlockSpec(memory_space=pltpu.VMEM)],
        out_specs=pl.BlockSpec(memory_space=pltpu.VMEM),
        scratch_shapes=[
            pltpu.VMEM((3, 8, 128), F32),
            pltpu.VMEM((7, 8, 128), F32),
            pltpu.SemaphoreType.DMA((7,)),
            pltpu.SemaphoreType.DMA((7,)),
        ],
        compiler_params=pltpu.CompilerParams(collective_id=0, has_side_effects=True),
        name="total",
    )(block)[0, 0]


def one_hot(rows, columns):
    return (rows[:, None] == columns[None, :]).astype(BF)


def feature_order():
    j = jnp.arange(D, dtype=jnp.int32)
    k = j - 1024
    return one_hot(j, jnp.where(j < 1024, (j // 32) * 36 + j % 32, (k // 4) * 36 + 32 + k % 4))


def rest_order():
    p, t = (jnp.arange(1024, dtype=jnp.int32) for _ in range(2))
    return one_hot((p % 32 // 4) * 128 + (p // 32) * 4 + p % 4, t)


def moved(a, order):
    return jnp.dot(a, order, preferred_element_type=F32).astype(BF)


def pack(gate, up, dn, order):
    main = [w[:32].reshape(32, Q, C).transpose(1, 0, 2).reshape(128, C) for w in (gate, up)]
    rest = [w[32:].reshape(4, Q, C).transpose(1, 0, 2).reshape(16, C) for w in (gate, up)]
    return jnp.concatenate(main + rest + [moved(dn, order)])


def unpack(g, order):
    out = []
    for i in range(2):
        main = g[128 * i : 128 * i + 128].reshape(Q, 32, C).transpose(1, 0, 2).reshape(32, FF)
        rest = g[256 + 16 * i : 272 + 16 * i].reshape(Q, 4, C).transpose(1, 0, 2).reshape(4, FF)
        out.append(jnp.concatenate([main, rest]))
    return out + [moved(g[288:], order.T)]


def adamw(w, m, v, g):
    m = 0.9 * m + 0.1 * g
    v = 0.95 * v + 0.05 * g * g
    step = m * lax.rsqrt(v + 1e-8) + 0.1 * w
    return (w - 0.02 * step).astype(BF), m, v


def across_kernel(a_ref, b_ref, c_ref, d_ref, out_ref):
    out_ref[...] = (a_ref[...].astype(F32) + b_ref[...].astype(F32) + c_ref[...].astype(F32) + d_ref[...].astype(F32)).astype(BF)


def across(block, n=4):
    others = [lax.ppermute(block, "r", [(i, (i + shift) % n) for i in range(n)]) for shift in range(1, n)]
    spec = pl.BlockSpec((144, C), lambda i: (i, 0))
    return pl.pallas_call(
        across_kernel,
        out_shape=jax.ShapeDtypeStruct(block.shape, BF),
        grid=(block.shape[0] // 144,),
        in_specs=[spec] * n,
        out_specs=spec,
        compiler_params=params(1),
        cost_estimate=cost(block.size * 4, block.size * 10),
        name="across",
    )(block, *others)


def scattered(term):
    return lax.psum_scatter(term.reshape(-1, C), "s", scatter_dimension=0, tiled=True)


def rest_of(packed, rests):
    return moved(rests.T, packed[:, 256:288, :].reshape(1024, C))


def solution(mesh):
    def step(x, dy, *arrays):
        weights, m, v = (arrays[i : i + 3] for i in (0, 3, 6))
        order, rests = feature_order(), rest_order()

        packed = [
            lax.all_gather(pack(*(w[n] for w in weights), order), "s", axis=0, tiled=True).reshape(S, ROWS, C)
            for n in range(2)
        ]

        x, dy = moved(x[0], order), moved(dy[0], order)
        a0 = normed_wide(x.astype(F32)).astype(BF)
        at0, packed[0] = lax.optimization_barrier((a0.T, packed[0]))
        rest = [rest_of(packed[0], rests)]
        act0 = gate_up(a0, packed[0], rest[0])
        h1, a1 = down(act0, packed[0], x)
        a1, at1, packed[1] = lax.optimization_barrier((a1, a1.T, packed[1]))
        rest.append(rest_of(packed[1], rests))
        act1, dgu1 = back(a1, dy, packed[1], rest[1], True)
        sum_down1 = scattered(d_down(act1, dy))
        term1 = d_gate_up(at1, dgu1, rests)
        sum1 = scattered(term1)
        dh1 = dstate(dgu1, packed[1], rest[1], h1, dy)
        sum_down0 = scattered(d_down(act0, dh1))
        _, dgu0 = back(a0, dh1, packed[0], rest[0], False)
        term0 = d_gate_up(at0, dgu0, rests)
        sum0 = scattered(term0)

        early = across(jnp.concatenate([sum1, sum_down1, sum_down0]))
        late = across(sum0)
        squares = summed_over_group(sum(jnp.sum(jnp.square(b.astype(F32))) for b in (early, late)))
        blocks = [jnp.concatenate([late, early[432:]]), early[:432]]
        factor = jnp.minimum(1.0, 0.5 * lax.rsqrt(squares / (2 * 3 * D * FF) + 1e-30))
        pieces = [unpack(b, order) for b in blocks]
        new = [
            adamw(weights[i].astype(F32), m[i], v[i], jnp.stack([pieces[n][i] for n in range(2)]).astype(F32) * factor)
            for i in range(3)
        ]
        return tuple(one[which] for which in range(3) for one in new)

    states, cut = P(("rep", "r", "s"), None, None), P(None, "s", None)
    step = jax.shard_map(
        step,
        mesh=mesh,
        in_specs=(states, states) + (cut,) * 9,
        out_specs=(P("rep", "s", None),) * 9,
        check_vma=False,
    )
    return step
```
